32 devices in a mesh: rep: 2 (over y), gx: 4 (over x, core), gy: 4 (over z).
Axes of the slice: x: 2, y: 2, z: 4, core: 2. Of those that a mesh axis runs over, the one named last changes fastest.
Arguments:
- deltas: bfloat16 [2, 2, 3584, 14336], P('rep', None, 'gx', 'gy'), may hold values from -32 to 32
- params: float32 [2, 4, 4, 2, 4, 4, 112, 896], P(None, None, 'gx', 'rep', None, 'gy'), may hold values from -0.75 to 0.75
- momentum: float32 [2, 4, 4, 2, 4, 4, 112, 896], P(None, None, 'gx', 'rep', None, 'gy'), may hold values from -1.5 to 1.5
Outputs:
- new_params: float32 [2, 4, 4, 2, 4, 4, 112, 896], P(None, None, 'gx', 'rep', None, 'gy')
- new_momentum: float32 [2, 4, 4, 2, 4, 4, 112, 896], P(None, None, 'gx', 'rep', None, 'gy')
The draws below stay inside these ranges and needn't reach their ends.
All inputs are finite; a program needn't handle non-finite values.
Results may differ from the reference program's by a relative error of at most 0.0003.
Values may be sent and summed in bfloat16 or wider, within the bound.
A program may use at most 128 MiB of HBM per device.

```python
import math
import jax
import jax.numpy as jnp
from jax import lax

D = 3584
FF = 14336
REPLICAS = 2
ROW_SPLIT = 4
COL_SPLIT = 4
ROW_TILE = 112
COL_TILE = 896


def draw_deltas(key, part):
    row_key, col_key, own_key = jax.random.split(key, 3)
    devices_all = REPLICAS * ROW_SPLIT * COL_SPLIT
    divisor = 2.0 * max(devices_all - 1, 1)
    rows_at = jnp.arange(D) % (D // ROW_SPLIT) // ROW_TILE
    rep_at = rows_at % REPLICAS
    gx_at = rows_at // REPLICAS
    cols_at = jnp.arange(FF) % (FF // COL_SPLIT) // COL_TILE
    row_ramp = jnp.exp(math.log(3.0) * (rep_at * ROW_SPLIT * COL_SPLIT + gx_at * COL_SPLIT).astype(jnp.float32) / divisor)
    col_ramp = jnp.exp(math.log(3.0) * cols_at.astype(jnp.float32) / divisor)
    row_scale = jnp.power(10.0, jax.random.uniform(row_key, (2, D, 1), jnp.float32)) * row_ramp[None, :, None]
    col_scale = jnp.power(10.0, jax.random.uniform(col_key, (2, 1, FF), jnp.float32)) * col_ramp[None, None, :]
    spread = 0.1 * row_scale * col_scale

    def draw_replica(replica):
        sample = jax.random.truncated_normal(jax.random.fold_in(own_key, replica), -6.0, 6.0, (2, D, FF), jnp.float32)
        value = jnp.clip(sample * spread, -32.0, 32.0)
        return value.astype(jnp.bfloat16)
    return lax.map(draw_replica, jnp.arange(REPLICAS))


def shard_levels(key, extent, pieces, low, top_value):
    def one(position, blocks):
        heights = jax.random.uniform(jax.random.fold_in(jax.random.fold_in(key, 6), position), (blocks,), jnp.float32, low / len(pieces), top_value / len(pieces))
        return jnp.repeat(jnp.exp(heights), extent[position] // blocks).reshape((-1,) + (1,) * (len(extent) - position - 1))

    loudness = one(*pieces[0])
    for cut in pieces[1:]:
        loudness = loudness * one(*cut)
    return loudness


def bell_draw(key, shape, width, reach, shards=(), kind=jnp.bfloat16):
    values = jax.random.normal(key, shape, jnp.float32) * width
    if len(shards) > 0:
        values = shard_levels(key, shape, shards, -0.22, 0.18) * values
    return jnp.clip(values, min=-reach, max=reach).astype(kind)


def setup_inputs(seed: int = 0) -> dict:
    seeds = jax.random.split(jax.random.key(seed), 4)
    return {
        "deltas": draw_deltas(jax.random.fold_in(seeds[3], 71), 0),
        "params": bell_draw(seeds[1], (2, ROW_SPLIT, ROW_SPLIT, REPLICAS, COL_SPLIT, COL_SPLIT, ROW_TILE, COL_TILE), 0.05, 0.75, ((2, 4), (3, 2), (5, 4)), jnp.float32),
        "momentum": bell_draw(seeds[2], (2, ROW_SPLIT, ROW_SPLIT, REPLICAS, COL_SPLIT, COL_SPLIT, ROW_TILE, COL_TILE), 0.1, 1.5, ((2, 4), (3, 2), (5, 4)), jnp.float32),
    }


clip_level = 0.25
moment_decay = 0.9
outer_rate = 0.7
epsilon = 1e-06

def reference(deltas, params, momentum):
    running = jnp.zeros(deltas.shape[1:], jnp.float32)
    for replica in range(REPLICAS):
        running = running + deltas[replica].astype(jnp.float32)
    mean_delta = running / REPLICAS
    squares = jnp.sum(mean_delta * mean_delta)
    entries = mean_delta.size
    root_mean = jnp.sqrt(squares / entries + epsilon)
    clip_scale = jnp.minimum(1.0, clip_level / root_mean)
    blocked = mean_delta.reshape(2, ROW_SPLIT, ROW_SPLIT, REPLICAS, ROW_TILE, COL_SPLIT, COL_SPLIT, COL_TILE)
    blocked = jnp.transpose(blocked, (0, 1, 2, 3, 5, 6, 4, 7))
    gradient = clip_scale * blocked
    new_momentum = moment_decay * momentum + gradient
    new_params = params - outer_rate * (gradient + moment_decay * new_momentum)
    return (new_params, new_momentum)
```

```python
import functools

import jax
import jax.numpy as jnp
from jax import lax
from jax.experimental import pallas as pl
from jax.experimental.pallas import tpu as pltpu
from jax.sharding import PartitionSpec as P

clip_level = 0.25
moment_decay = 0.9
outer_rate = 0.7
epsilon = 1e-06

MESH = pl.DeviceIdType.MESH
LANES = 128
TOP = 240.0
SMALLEST = 1e-30
AHEAD = 6


def encode(value):
    power = value * value
    for _ in range(3):
        power = power * power
    return jnp.where(value < 0.0, -power, power).astype(jnp.bfloat16)


def decode(code):
    wide = code.astype(jnp.float32)
    root = jnp.abs(wide)
    for _ in range(4):
        root = lax.rsqrt(root)
    root = jnp.where(wide == 0.0, 0.0, root)
    return jnp.where(wide < 0.0, -root, root)


def fold_lanes(tile, combine):
    folded = tile[:, :LANES]
    for start in range(LANES, tile.shape[1], LANES):
        folded = combine(folded, tile[:, start : start + LANES])
    return folded


def exchange(
    replicas, rows_split, cols_split, matrices,
    delta_ref, tiles_ref, peaks_ref, squares_ref,
    own, peer, stage, peaks, wide, total, mine, from_rep, middle, from_grid,
    own_sem, rep_send, rep_recv, tile_send, tile_recv, peak_send, peak_recv,
    first_send, first_recv, second_send, second_recv, local_sem,
):
    rep, gx, gy = lax.axis_index("rep"), lax.axis_index("gx"), lax.axis_index("gy")
    steps, rows, cols = stage.shape
    grid = rows_split * cols_split
    far = rows_split * (cols_split - 1)
    remote_steps = steps - matrices
    band = total.shape[0]
    here = gx * cols_split + gy

    def place(step):
        turn, matrix = step // matrices, step % matrices
        spread = max(cols_split - 1, 1)
        is_far = turn < far
        row_shift = jnp.where(is_far, turn // spread, (turn - far + 1) % rows_split)
        col_shift = jnp.where(is_far, 1 + (turn % spread + 1) % spread, 0)
        return matrix, (gx + row_shift) % rows_split, (gy + col_shift) % cols_split

    def block(step, replica):
        matrix, c, d = place(step)
        return delta_ref.at[matrix, c, replica, :, pl.ds(pl.multiple_of(d * cols, LANES), cols)]

    def own_copy(step):
        return pltpu.make_async_copy(block(step, rep), own.at[step], own_sem.at[step])

    def rep_copy(shift, step):
        target = (rep + shift) % replicas
        return pltpu.make_async_remote_copy(
            src_ref=block(step, target), dst_ref=peer.at[shift - 1, step],
            send_sem=rep_send.at[shift - 1, step], recv_sem=rep_recv.at[shift - 1, step],
            device_id={"rep": target}, device_id_type=MESH,
        )

    def tile_copies(step):
        matrix, c, d = place(step)
        slot = here * matrices + matrix
        target = {"gx": c, "gy": d}
        return (
            pltpu.make_async_remote_copy(
                src_ref=stage.at[step], dst_ref=tiles_ref.at[matrix, gx, gy],
                send_sem=tile_send.at[step], recv_sem=tile_recv.at[slot],
                device_id=target, device_id_type=MESH,
            ),
            pltpu.make_async_remote_copy(
                src_ref=peaks.at[step], dst_ref=peaks_ref.at[matrix, gx, gy],
                send_sem=peak_send.at[step], recv_sem=peak_recv.at[slot],
                device_id=target, device_id_type=MESH,
            ),
        )

    def neighbour(shift):
        return (gx + shift // cols_split) % rows_split, (gy + shift % cols_split) % cols_split

    barrier = pltpu.get_barrier_semaphore()
    for shift in range(1, replicas):
        pl.semaphore_signal(
            barrier, inc=1, device_id={"rep": (rep + shift) % replicas}, device_id_type=MESH
        )

    def greet(shift, carry):
        c, d = neighbour(shift)
        pl.semaphore_signal(barrier, inc=1, device_id={"gx": c, "gy": d}, device_id_type=MESH)
        return carry

    lax.fori_loop(1, grid, greet, 0)
    pl.semaphore_wait(barrier, replicas - 1 + grid - 1)

    def launch(step):
        own_copy(step).start()
        for shift in range(1, replicas):
            rep_copy(shift, step).start()

    ahead = min(AHEAD, steps)
    lax.fori_loop(0, ahead, lambda step, carry: (launch(step), carry)[1], 0)
    total[...] = jnp.zeros_like(total)

    def advance(step, carry):
        own_copy(step).wait()
        for shift in range(1, replicas):
            rep_copy(shift, step).wait_recv()

        @pl.when(step + ahead < steps)
        def _():
            launch(step + ahead)

        @pl.when((step >= 1) & (step - 1 < remote_steps))
        def _():
            for copy in tile_copies(step - 1):
                copy.start()

        def average(index, peak):
            at = pl.ds(pl.multiple_of(index * band, band), band)
            value = own[step, at, :].astype(jnp.float32)
            for shift in range(1, replicas):
                value = value + peer[shift - 1, step, at, :].astype(jnp.float32)
            value = value * (1.0 / replicas)
            total[...] += value * value
            wide[at, :] = value
            return jnp.maximum(peak, fold_lanes(jnp.abs(value), jnp.maximum))

        peak = lax.fori_loop(0, rows // band, average, jnp.zeros((band, LANES), jnp.float32))
        peak = jnp.maximum(jnp.max(peak, axis=0, keepdims=True), SMALLEST)
        peaks[step] = peak * (1.0 / TOP)
        lift = jnp.concatenate([TOP / peak] * (cols // LANES), axis=1)

        def code(index, carry):
            at = pl.ds(pl.multiple_of(index * band, band), band)
            stage[step, at, :] = encode(wide[at, :] * lift)
            return carry

        lax.fori_loop(0, rows // band, code, 0)
        return carry

    lax.fori_loop(0, steps, advance, 0)

    mine[...] = jnp.sum(fold_lanes(total[...], jnp.add), axis=0, keepdims=True)

    def local_copies(matrix):
        step = remote_steps + matrix
        return (
            pltpu.make_async_copy(stage.at[step], tiles_ref.at[matrix, gx, gy], local_sem.at[matrix, 0]),
            pltpu.make_async_copy(peaks.at[step], peaks_ref.at[matrix, gx, gy], local_sem.at[matrix, 1]),
        )

    def first_copy(shift):
        return pltpu.make_async_remote_copy(
            src_ref=mine, dst_ref=from_rep.at[shift - 1],
            send_sem=first_send.at[shift - 1], recv_sem=first_recv.at[shift - 1],
            device_id={"rep": (rep + shift) % replicas}, device_id_type=MESH,
        )

    def second_copy(shift):
        c, d = neighbour(shift)
        return pltpu.make_async_remote_copy(
            src_ref=middle, dst_ref=from_grid.at[shift - 1],
            send_sem=second_send.at[shift - 1], recv_sem=second_recv.at[shift - 1],
            device_id={"gx": c, "gy": d}, device_id_type=MESH,
        )

    for matrix in range(matrices):
        for copy in local_copies(matrix):
            copy.start()
    for shift in range(1, replicas):
        first_copy(shift).start()
    for matrix in range(matrices):
        for copy in local_copies(matrix):
            copy.wait()
    subtotal = mine[...]
    for shift in range(1, replicas):
        first_copy(shift).wait()
        subtotal = subtotal + from_rep[shift - 1]
    middle[...] = subtotal

    def close_rep(step, carry):
        for shift in range(1, replicas):
            rep_copy(shift, step).wait_send()
        return carry

    lax.fori_loop(0, steps, close_rep, 0)
    lax.fori_loop(1, grid, lambda shift, carry: (second_copy(shift).start(), carry)[1], 0)

    def gather(shift, carry):
        second_copy(shift).wait()
        return carry + from_grid[shift - 1]

    squares_ref[...] = lax.fori_loop(1, grid, gather, subtotal)

    def close_send(step, carry):
        for copy in tile_copies(step):
            copy.wait_send()
        return carry

    lax.fori_loop(0, remote_steps, close_send, 0)

    def close_recv(index, carry):
        c, d = neighbour(1 + index // matrices)
        matrix = index % matrices
        slot = (c * cols_split + d) * matrices + matrix
        target = {"gx": c, "gy": d}
        pltpu.make_async_remote_copy(
            src_ref=stage.at[0], dst_ref=tiles_ref.at[matrix, c, d],
            send_sem=tile_send.at[0], recv_sem=tile_recv.at[slot],
            device_id=target, device_id_type=MESH,
        ).wait_recv()
        pltpu.make_async_remote_copy(
            src_ref=peaks.at[0], dst_ref=peaks_ref.at[matrix, c, d],
            send_sem=peak_send.at[0], recv_sem=peak_recv.at[slot],
            device_id=target, device_id_type=MESH,
        ).wait_recv()
        return carry

    lax.fori_loop(0, remote_steps, close_recv, 0)


def update(entries, squares_ref, tiles_ref, peaks_ref, params_ref, momentum_ref, new_params_ref, new_momentum_ref):
    squares = jnp.sum(squares_ref[...], axis=1, keepdims=True)
    clip_scale = jnp.minimum(1.0, clip_level / jnp.sqrt(squares / entries + epsilon))
    count, rows, cols = tiles_ref.shape
    band = 16 if rows % 16 == 0 else rows
    for tile in range(count):
        lift = jnp.concatenate([peaks_ref[tile] * clip_scale] * (cols // LANES), axis=1)

        def one(index, carry):
            at = pl.ds(pl.multiple_of(index * band, band), band)
            gradient = decode(tiles_ref[tile, at, :]) * lift
            new_momentum = moment_decay * momentum_ref[tile, at, :] + gradient
            new_momentum_ref[tile, at, :] = new_momentum
            new_params_ref[tile, at, :] = params_ref[tile, at, :] - outer_rate * (
                gradient + moment_decay * new_momentum
            )
            return carry

        lax.fori_loop(0, rows // band, one, 0)


def per_device(deltas, params, momentum):
    rows_split = lax.axis_size("gx")
    cols_split = lax.axis_size("gy")
    replicas = lax.axis_size("rep")
    matrices, local_rows, local_cols = deltas.shape[1:]
    rows = local_rows // (rows_split * replicas)
    cols = local_cols // cols_split
    entries = matrices * local_rows * local_cols * rows_split * cols_split
    grid = rows_split * cols_split
    steps = grid * matrices
    remote_steps = steps - matrices
    band = 16 if rows % 16 == 0 else rows
    any_space = pl.BlockSpec(memory_space=pl.ANY)
    vmem = pl.BlockSpec(memory_space=pltpu.VMEM)
    dma = pltpu.SemaphoreType.DMA
    f32, bf16 = jnp.float32, jnp.bfloat16
    padded = -(-rows // 16) * 16
    buffers = (replicas + 1) * steps * padded * cols * 2
    tiles, peaks, squares = pl.pallas_call(
        functools.partial(exchange, replicas, rows_split, cols_split, matrices),
        out_shape=(
            jax.ShapeDtypeStruct((matrices, rows_split, cols_split, rows, cols), bf16),
            jax.ShapeDtypeStruct((matrices, rows_split, cols_split, 1, LANES), f32),
            jax.ShapeDtypeStruct((1, LANES), f32),
        ),
        in_specs=[any_space],
        out_specs=(any_space, any_space, vmem),
        scratch_shapes=[
            pltpu.VMEM((steps, rows, cols), bf16),
            pltpu.VMEM((max(replicas - 1, 1), steps, rows, cols), bf16),
            pltpu.VMEM((steps, rows, cols), bf16),
            pltpu.VMEM((steps, 1, LANES), f32),
            pltpu.VMEM((rows, cols), f32),
            pltpu.VMEM((band, cols), f32),
            pltpu.VMEM((1, LANES), f32),
            pltpu.VMEM((max(replicas - 1, 1), 1, LANES), f32),
            pltpu.VMEM((1, LANES), f32),
            pltpu.VMEM((grid, 1, LANES), f32),
            dma((steps,)),
            dma((max(replicas - 1, 1), steps)),
            dma((max(replicas - 1, 1), steps)),
            dma((steps,)),
            dma((steps,)),
            dma((steps,)),
            dma((steps,)),
            dma((max(replicas - 1, 1),)),
            dma((max(replicas - 1, 1),)),
            dma((grid,)),
            dma((grid,)),
            dma((matrices, 2)),
        ],
        compiler_params=pltpu.CompilerParams(
            collective_id=0, has_side_effects=True, vmem_limit_bytes=buffers + 6 * 1024 * 1024
        ),
    )(deltas.reshape(matrices, rows_split, replicas, rows, local_cols))
    tile_shape = (steps, rows, cols)
    count = 2 if steps % 2 == 0 else 1
    whole = pl.BlockSpec((1, LANES), lambda i: (0, 0))
    tile_block = pl.BlockSpec((count, rows, cols), lambda i: (i, 0, 0))
    peak_block = pl.BlockSpec((count, 1, LANES), lambda i: (i, 0, 0))
    wide_shape = jax.ShapeDtypeStruct(tile_shape, f32)
    new_params, new_momentum = pl.pallas_call(
        functools.partial(update, entries),
        grid=(steps // count,),
        out_shape=(wide_shape, wide_shape),
        in_specs=[whole, tile_block, peak_block, tile_block, tile_block],
        out_specs=(tile_block, tile_block),
        compiler_params=pltpu.CompilerParams(vmem_limit_bytes=16 * 1024 * 1024),
    )(
        squares,
        tiles.reshape(tile_shape),
        peaks.reshape(steps, 1, LANES),
        params.reshape(tile_shape),
        momentum.reshape(tile_shape),
    )
    return (new_params.reshape(params.shape), new_momentum.reshape(momentum.shape))


def solution(mesh):
    placement = P(None, None, "gx", "rep", None, "gy", None, None)
    return jax.shard_map(
        per_device,
        mesh=mesh,
        in_specs=(P("rep", None, "gx", "gy"), placement, placement),
        out_specs=(placement, placement),
        check_vma=False,
    )
```

```python
import functools

import jax
import jax.numpy as jnp
from jax import lax
from jax.experimental import pallas as pl
from jax.experimental.pallas import tpu as pltpu
from jax.sharding import PartitionSpec as P

clip_level = 0.25
moment_decay = 0.9
outer_rate = 0.7
epsilon = 1e-06

MESH = pl.DeviceIdType.MESH
LANES = 128
TOP = 240.0
SMALLEST = 1e-30
AHEAD = 16
LARGE = 54 * 1024 * 1024


def encode(value):
    power = value * value
    for _ in range(3):
        power = power * power
    return jnp.where(value < 0.0, -power, power).astype(jnp.bfloat16)


def decode(code):
    wide = code.astype(jnp.float32)
    root = jnp.exp2(jnp.log2(jnp.abs(wide)) * (1.0 / 16.0))
    root = jnp.where(wide == 0.0, 0.0, root)
    return jnp.where(wide < 0.0, -root, root)


def fold_lanes(tile, combine):
    folded = tile[:, :LANES]
    for start in range(LANES, tile.shape[1], LANES):
        folded = combine(folded, tile[:, start : start + LANES])
    return folded


def exchange(
    replicas, rows_split, cols_split, matrices,
    delta_ref, tiles_ref, peaks_ref, squares_ref,
    own, peer, stage, peaks, wide, total, mine, from_rep, middle, from_grid,
    own_sem, rep_send, rep_recv, tile_send, tile_recv, peak_send, peak_recv,
    first_send, first_recv, second_send, second_recv, local_sem,
):
    rep, gx, gy = lax.axis_index("rep"), lax.axis_index("gx"), lax.axis_index("gy")
    steps, rows, cols = stage.shape
    grid = rows_split * cols_split
    far = rows_split * (cols_split - 1)
    remote_steps = steps - matrices
    band = total.shape[0]
    here = gx * cols_split + gy

    def place(step):
        turn, matrix = step // matrices, step % matrices
        spread = max(cols_split - 1, 1)
        is_far = turn < far
        row_shift = jnp.where(is_far, turn // spread, (turn - far + 1) % rows_split)
        col_shift = jnp.where(is_far, 1 + (turn % spread + 1) % spread, 0)
        return matrix, (gx + row_shift) % rows_split, (gy + col_shift) % cols_split

    def block(step, replica):
        matrix, c, d = place(step)
        return delta_ref.at[matrix, c, replica, :, pl.ds(pl.multiple_of(d * cols, LANES), cols)]

    def own_copy(step):
        return pltpu.make_async_copy(block(step, rep), own.at[step], own_sem.at[step])

    def rep_copy(shift, step):
        target = (rep + shift) % replicas
        return pltpu.make_async_remote_copy(
            src_ref=block(step, target), dst_ref=peer.at[shift - 1, step],
            send_sem=rep_send.at[shift - 1, step], recv_sem=rep_recv.at[shift - 1, step],
            device_id={"rep": target}, device_id_type=MESH,
        )

    def tile_copies(step):
        matrix, c, d = place(step)
        slot = here * matrices + matrix
        target = {"gx": c, "gy": d}
        return (
            pltpu.make_async_remote_copy(
                src_ref=stage.at[step], dst_ref=tiles_ref.at[matrix, gx, gy],
                send_sem=tile_send.at[step], recv_sem=tile_recv.at[slot],
                device_id=target, device_id_type=MESH,
            ),
            pltpu.make_async_remote_copy(
                src_ref=peaks.at[step], dst_ref=peaks_ref.at[matrix, gx, gy],
                send_sem=peak_send.at[step], recv_sem=peak_recv.at[slot],
                device_id=target, device_id_type=MESH,
            ),
        )

    def neighbour(shift):
        return (gx + shift // cols_split) % rows_split, (gy + shift % cols_split) % cols_split

    barrier = pltpu.get_barrier_semaphore()
    for shift in range(1, replicas):
        pl.semaphore_signal(
            barrier, inc=1, device_id={"rep": (rep + shift) % replicas}, device_id_type=MESH
        )

    def greet(shift, carry):
        c, d = neighbour(shift)
        pl.semaphore_signal(barrier, inc=1, device_id={"gx": c, "gy": d}, device_id_type=MESH)
        return carry

    lax.fori_loop(1, grid, greet, 0)
    pl.semaphore_wait(barrier, replicas - 1 + grid - 1)

    def launch(step):
        own_copy(step).start()
        for shift in range(1, replicas):
            rep_copy(shift, step).start()

    ahead = min(AHEAD, steps)
    lax.fori_loop(0, ahead, lambda step, carry: (launch(step), carry)[1], 0)
    total[...] = jnp.zeros_like(total)

    def advance(step, carry):
        own_copy(step).wait()
        for shift in range(1, replicas):
            rep_copy(shift, step).wait_recv()

        @pl.when(step + ahead < steps)
        def _():
            launch(step + ahead)

        def average(index, peak):
            at = pl.ds(pl.multiple_of(index * band, band), band)
            value = own[step, at, :].astype(jnp.float32)
            for shift in range(1, replicas):
                value = value + peer[shift - 1, step, at, :].astype(jnp.float32)
            value = value * (1.0 / replicas)
            total[...] += value * value
            wide[at, :] = value
            return jnp.maximum(peak, fold_lanes(jnp.abs(value), jnp.maximum))

        peak = lax.fori_loop(0, rows // band, average, jnp.zeros((band, LANES), jnp.float32))
        peak = jnp.maximum(jnp.max(peak, axis=0, keepdims=True), SMALLEST)
        peaks[step] = peak * (1.0 / TOP)
        lift = jnp.concatenate([TOP / peak] * (cols // LANES), axis=1)

        def code(index, carry):
            at = pl.ds(pl.multiple_of(index * band, band), band)
            stage[step, at, :] = encode(wide[at, :] * lift)
            return carry

        lax.fori_loop(0, rows // band, code, 0)

        @pl.when(step < remote_steps)
        def _():
            for copy in tile_copies(step):
                copy.start()

        return carry

    lax.fori_loop(0, steps, advance, 0)

    mine[...] = jnp.sum(fold_lanes(total[...], jnp.add), axis=0, keepdims=True)

    def local_copies(matrix):
        step = remote_steps + matrix
        return (
            pltpu.make_async_copy(stage.at[step], tiles_ref.at[matrix, gx, gy], local_sem.at[matrix, 0]),
            pltpu.make_async_copy(peaks.at[step], peaks_ref.at[matrix, gx, gy], local_sem.at[matrix, 1]),
        )

    def first_copy(shift):
        return pltpu.make_async_remote_copy(
            src_ref=mine, dst_ref=from_rep.at[shift - 1],
            send_sem=first_send.at[shift - 1], recv_sem=first_recv.at[shift - 1],
            device_id={"rep": (rep + shift) % replicas}, device_id_type=MESH,
        )

    def second_copy(shift):
        c, d = neighbour(shift)
        return pltpu.make_async_remote_copy(
            src_ref=middle, dst_ref=from_grid.at[shift - 1],
            send_sem=second_send.at[shift - 1], recv_sem=second_recv.at[shift - 1],
            device_id={"gx": c, "gy": d}, device_id_type=MESH,
        )

    for matrix in range(matrices):
        for copy in local_copies(matrix):
            copy.start()
    for shift in range(1, replicas):
        first_copy(shift).start()
    for matrix in range(matrices):
        for copy in local_copies(matrix):
            copy.wait()
    subtotal = mine[...]
    for shift in range(1, replicas):
        first_copy(shift).wait()
        subtotal = subtotal + from_rep[shift - 1]
    middle[...] = subtotal

    def close_rep(step, carry):
        for shift in range(1, replicas):
            rep_copy(shift, step).wait_send()
        return carry

    lax.fori_loop(0, steps, close_rep, 0)
    lax.fori_loop(1, grid, lambda shift, carry: (second_copy(shift).start(), carry)[1], 0)

    def gather(shift, carry):
        second_copy(shift).wait()
        return carry + from_grid[shift - 1]

    squares_ref[...] = lax.fori_loop(1, grid, gather, subtotal)

    def close_send(step, carry):
        for copy in tile_copies(step):
            copy.wait_send()
        return carry

    lax.fori_loop(0, remote_steps, close_send, 0)

    def close_recv(index, carry):
        c, d = neighbour(1 + index // matrices)
        matrix = index % matrices
        slot = (c * cols_split + d) * matrices + matrix
        target = {"gx": c, "gy": d}
        pltpu.make_async_remote_copy(
            src_ref=stage.at[0], dst_ref=tiles_ref.at[matrix, c, d],
            send_sem=tile_send.at[0], recv_sem=tile_recv.at[slot],
            device_id=target, device_id_type=MESH,
        ).wait_recv()
        pltpu.make_async_remote_copy(
            src_ref=peaks.at[0], dst_ref=peaks_ref.at[matrix, c, d],
            send_sem=peak_send.at[0], recv_sem=peak_recv.at[slot],
            device_id=target, device_id_type=MESH,
        ).wait_recv()
        return carry

    lax.fori_loop(0, remote_steps, close_recv, 0)


def update(entries, squares_ref, tiles_ref, peaks_ref, params_ref, momentum_ref, new_params_ref, new_momentum_ref):
    squares = jnp.sum(squares_ref[...], axis=1, keepdims=True)
    clip_scale = jnp.minimum(1.0, clip_level / jnp.sqrt(squares / entries + epsilon))
    count, rows, cols = tiles_ref.shape
    band = 16 if rows % 16 == 0 else rows
    for tile in range(count):
        lift = jnp.concatenate([peaks_ref[tile] * clip_scale] * (cols // LANES), axis=1)

        for start in range(0, rows, band):
            at = slice(start, start + band)
            gradient = decode(tiles_ref[tile, at, :]) * lift
            new_momentum = moment_decay * momentum_ref[tile, at, :] + gradient
            new_momentum_ref[tile, at, :] = new_momentum
            new_params_ref[tile, at, :] = params_ref[tile, at, :] - outer_rate * (
                gradient + moment_decay * new_momentum
            )


def per_device(deltas, params, momentum):
    rows_split = lax.axis_size("gx")
    cols_split = lax.axis_size("gy")
    replicas = lax.axis_size("rep")
    matrices, local_rows, local_cols = deltas.shape[1:]
    rows = local_rows // (rows_split * replicas)
    cols = local_cols // cols_split
    entries = matrices * local_rows * local_cols * rows_split * cols_split
    grid = rows_split * cols_split
    steps = grid * matrices
    remote_steps = steps - matrices
    band = 16 if rows % 16 == 0 else rows
    any_space = pl.BlockSpec(memory_space=pl.ANY)
    vmem = pl.BlockSpec(memory_space=pltpu.VMEM)
    dma = pltpu.SemaphoreType.DMA
    f32, bf16 = jnp.float32, jnp.bfloat16
    tiles, peaks, squares = pl.pallas_call(
        functools.partial(exchange, replicas, rows_split, cols_split, matrices),
        out_shape=(
            jax.ShapeDtypeStruct((matrices, rows_split, cols_split, rows, cols), bf16),
            jax.ShapeDtypeStruct((matrices, rows_split, cols_split, 1, LANES), f32),
            jax.ShapeDtypeStruct((1, LANES), f32),
        ),
        in_specs=[any_space],
        out_specs=(any_space, any_space, vmem),
        scratch_shapes=[
            pltpu.VMEM((steps, rows, cols), bf16),
            pltpu.VMEM((max(replicas - 1, 1), steps, rows, cols), bf16),
            pltpu.VMEM((steps, rows, cols), bf16),
            pltpu.VMEM((steps, 1, LANES), f32),
            pltpu.VMEM((rows, cols), f32),
            pltpu.VMEM((band, cols), f32),
            pltpu.VMEM((1, LANES), f32),
            pltpu.VMEM((max(replicas - 1, 1), 1, LANES), f32),
            pltpu.VMEM((1, LANES), f32),
            pltpu.VMEM((grid, 1, LANES), f32),
            dma((steps,)),
            dma((max(replicas - 1, 1), steps)),
            dma((max(replicas - 1, 1), steps)),
            dma((steps,)),
            dma((steps,)),
            dma((steps,)),
            dma((steps,)),
            dma((max(replicas - 1, 1),)),
            dma((max(replicas - 1, 1),)),
            dma((grid,)),
            dma((grid,)),
            dma((matrices, 2)),
        ],
        compiler_params=pltpu.CompilerParams(
            collective_id=0, has_side_effects=True, vmem_limit_bytes=LARGE
        ),
    )(deltas.reshape(matrices, rows_split, replicas, rows, local_cols))
    tile_shape = (steps, rows, cols)
    count = 2 if steps % 2 == 0 else 1
    whole = pl.BlockSpec((1, LANES), lambda i: (0, 0))
    tile_block = pl.BlockSpec((count, rows, cols), lambda i: (i, 0, 0))
    peak_block = pl.BlockSpec((count, 1, LANES), lambda i: (i, 0, 0))
    wide_shape = jax.ShapeDtypeStruct(tile_shape, f32)
    new_params, new_momentum = pl.pallas_call(
        functools.partial(update, entries),
        grid=(steps // count,),
        out_shape=(wide_shape, wide_shape),
        in_specs=[whole, tile_block, peak_block, tile_block, tile_block],
        out_specs=(tile_block, tile_block),
        compiler_params=pltpu.CompilerParams(vmem_limit_bytes=LARGE),
    )(
        squares,
        tiles.reshape(tile_shape),
        peaks.reshape(steps, 1, LANES),
        params.reshape(tile_shape),
        momentum.reshape(tile_shape),
    )
    return (new_params.reshape(params.shape), new_momentum.reshape(momentum.shape))


def solution(mesh):
    placement = P(None, None, "gx", "rep", None, "gy", None, None)
    return jax.shard_map(
        per_device,
        mesh=mesh,
        in_specs=(P("rep", None, "gx", "gy"), placement, placement),
        out_specs=(placement, placement),
        check_vma=False,
    )
```
